32 devices in a mesh: dp: 2 (over x), pp: 4 (over z), sp: 4 (over y, core).
Axes of the slice: x: 2, y: 2, z: 4, core: 2. Of those that a mesh axis runs over, the one named last changes fastest.
Arguments:
- latent_in: float32 [4, 512, 16], P('dp', 'sp'), parts along dimension 0
- pos_embed: bfloat16 [2, 512, 1152], P(None, 'sp')
- condition: bfloat16 [4, 1152], P('dp'), parts along dimension 0
- step_size: float32 [4], P('dp'), parts along dimension 0
- w_in: bfloat16 [16, 1152], replicated
- w_ada: bfloat16 [8, 1152, 6912], replicated
- w_qkv: bfloat16 [8, 1152, 3456], replicated
- w_o: bfloat16 [8, 1152, 1152], replicated
- w_up: bfloat16 [8, 1152, 4608], replicated
- w_down: bfloat16 [8, 4608, 1152], replicated
- b_layer: bfloat16 [8, 17280], replicated
- w_fa: bfloat16 [1152, 2304], replicated
- b_fa: bfloat16 [2304], replicated
- w_out: bfloat16 [1152, 16], replicated
- k_old: bfloat16 [16, 1024, 16, 72], P('dp'), parts along dimension 0
- v_old: bfloat16 [16, 1024, 16, 72], P('dp'), parts along dimension 0
Outputs:
- output: float32 [4, 512, 16], P('dp', 'sp'), parts along dimension 0
There are 2 independent parts. The reference program is written for one: setup_inputs(seed, part) draws one part's arguments, and reference() takes and returns one part's arrays. A program takes and returns all parts, laid end to end along the dimension named above; an argument that names none is the same for every part.
All inputs are finite; a program needn't handle non-finite values.
Results may differ from the reference program's by a relative error of at most 0.0134576.
Values are sent between devices in bfloat16 or wider.
A program may use at most 1.75 GiB of HBM per device.

```python
import jax
import jax.numpy as jnp
from jax import lax
import math

TOKENS = 1024
PATCHES = 2
WIDTH = 1152
HEADS = 16
PATCH_DIM = 16
LAYERS = 8

PATCH_ROWS = TOKENS // PATCHES
HEAD_DIM = WIDTH // HEADS
LN_EPS = 1e-6


def setup_inputs(seed: int = 0, part: int = 0) -> dict:
    own_keys = jax.random.split(jax.random.fold_in(jax.random.key(seed), part), 7)
    shared_keys = jax.random.split(jax.random.key(seed + 1), 11)
    width_scale = WIDTH ** -0.5
    qk_boost = (math.log(TOKENS / 6.0) / 2.9) ** 0.25
    column_gain = jnp.concatenate([jnp.full((2 * WIDTH,), qk_boost, jnp.float32), jnp.ones((WIDTH,), jnp.float32)])
    buf_shape = (LAYERS, TOKENS, HEADS, HEAD_DIM)
    mean_shape = (LAYERS, 1, HEADS, HEAD_DIM)
    latent_in = jax.random.normal(own_keys[0], (PATCHES, PATCH_ROWS, PATCH_DIM), jnp.float32)
    condition = jax.random.normal(own_keys[1], (2, WIDTH), jnp.float32).astype(jnp.bfloat16)
    step_size = jax.random.uniform(own_keys[2], (2,), jnp.float32, 0.6, 1.2)
    key_mean = 0.7 * jax.random.normal(own_keys[3], mean_shape, jnp.float32)
    k_old = (1.2 * qk_boost * jax.random.normal(own_keys[4], buf_shape, jnp.float32) + key_mean).astype(jnp.bfloat16)
    value_mean = jax.random.normal(own_keys[5], mean_shape, jnp.float32)
    v_old = (jax.random.normal(own_keys[6], buf_shape, jnp.float32) + value_mean).astype(jnp.bfloat16)
    pos_embed = (0.7 * jax.random.normal(shared_keys[0], (PATCHES, PATCH_ROWS, WIDTH), jnp.float32)).astype(jnp.bfloat16)
    w_in = (jax.random.normal(shared_keys[1], (PATCH_DIM, WIDTH), jnp.float32) * PATCH_DIM ** -0.5).astype(jnp.bfloat16)
    w_ada = (jax.random.normal(shared_keys[2], (LAYERS, WIDTH, 6 * WIDTH), jnp.float32) * width_scale).astype(jnp.bfloat16)
    w_qkv = (jax.random.normal(shared_keys[3], (LAYERS, WIDTH, 3 * WIDTH), jnp.float32) * width_scale * column_gain).astype(jnp.bfloat16)
    w_o = (jax.random.normal(shared_keys[4], (LAYERS, WIDTH, WIDTH), jnp.float32) * width_scale).astype(jnp.bfloat16)
    w_up = (jax.random.normal(shared_keys[5], (LAYERS, WIDTH, 4 * WIDTH), jnp.float32) * width_scale).astype(jnp.bfloat16)
    w_down = (jax.random.normal(shared_keys[6], (LAYERS, 4 * WIDTH, WIDTH), jnp.float32) * (4 * WIDTH) ** -0.5).astype(jnp.bfloat16)
    b_layer = (0.3 * jax.random.normal(shared_keys[7], (LAYERS, 15 * WIDTH), jnp.float32)).astype(jnp.bfloat16)
    w_fa = (jax.random.normal(shared_keys[8], (WIDTH, 2 * WIDTH), jnp.float32) * width_scale).astype(jnp.bfloat16)
    b_fa = (0.3 * jax.random.normal(shared_keys[9], (2 * WIDTH,), jnp.float32)).astype(jnp.bfloat16)
    w_out = (jax.random.normal(shared_keys[10], (WIDTH, PATCH_DIM), jnp.float32) * width_scale).astype(jnp.bfloat16)
    return {"latent_in": latent_in, "pos_embed": pos_embed, "condition": condition, "step_size": step_size, "w_in": w_in, "w_ada": w_ada, "w_qkv": w_qkv, "w_o": w_o, "w_up": w_up, "w_down": w_down, "b_layer": b_layer, "w_fa": w_fa, "b_fa": b_fa, "w_out": w_out, "k_old": k_old, "v_old": v_old}


def layer_norm(hidden):
    mean_val = jnp.mean(hidden, axis=-1, keepdims=True)
    centered = hidden - mean_val
    var_val = jnp.mean(centered * centered, axis=-1, keepdims=True)
    return centered * lax.rsqrt(var_val + LN_EPS)


def attend_head(operands):
    query_head, key_head, value_head = operands
    logits = jnp.dot(query_head, key_head.T, preferred_element_type=jnp.float32) * HEAD_DIM ** -0.5
    attn_prob = jax.nn.softmax(logits, axis=-1).astype(jnp.bfloat16)
    return jnp.dot(attn_prob, value_head, preferred_element_type=jnp.float32).astype(jnp.bfloat16)


def reference(latent_in, pos_embed, condition, step_size, w_in, w_ada, w_qkv, w_o, w_up, w_down, b_layer, w_fa, b_fa, w_out, k_old, v_old):
    bias_f32 = b_layer.astype(jnp.float32)
    key_bufs = k_old
    value_bufs = v_old
    latent = latent_in
    for step_idx in range(2):
        cond_act = jax.nn.silu(condition[step_idx].astype(jnp.float32)).astype(jnp.bfloat16)
        mod_all = jnp.einsum("c,lcf->lf", cond_act.astype(jnp.float32), w_ada.astype(jnp.float32)) + bias_f32[:, :6 * WIDTH]
        final_mod = jnp.dot(cond_act[None, :], w_fa, preferred_element_type=jnp.float32)[0] + b_fa.astype(jnp.float32)
        scale_out, shift_out = jnp.split(final_mod, 2)
        step_val = step_size[step_idx]
        latent_now = latent

        def patch_body(buffers, patch_idx):
            key_all, value_all = buffers
            row_start = patch_idx * PATCH_ROWS
            x_patch = latent_now[patch_idx]

            def block(hidden, layer_in):
                mod_vec, qkv_weight, out_weight, up_weight, down_weight, bias_row, key_buf, value_buf = layer_in
                scale_attn, shift_attn, gate_attn, scale_mlp, shift_mlp, gate_mlp = jnp.split(mod_vec, 6)
                normed = (layer_norm(hidden.astype(jnp.float32)) * (1.0 + scale_attn) + shift_attn).astype(jnp.bfloat16)
                qkv_rows = (jnp.dot(normed, qkv_weight, preferred_element_type=jnp.float32) + bias_row[6 * WIDTH:9 * WIDTH]).astype(jnp.bfloat16)
                query_rows = qkv_rows[:, :WIDTH].reshape(PATCH_ROWS, HEADS, HEAD_DIM)
                key_buf = lax.dynamic_update_slice_in_dim(key_buf, qkv_rows[:, WIDTH:2 * WIDTH].reshape(PATCH_ROWS, HEADS, HEAD_DIM), row_start, axis=0)
                value_buf = lax.dynamic_update_slice_in_dim(value_buf, qkv_rows[:, 2 * WIDTH:].reshape(PATCH_ROWS, HEADS, HEAD_DIM), row_start, axis=0)
                attn_heads = lax.map(attend_head, (jnp.transpose(query_rows, (1, 0, 2)), jnp.transpose(key_buf, (1, 0, 2)), jnp.transpose(value_buf, (1, 0, 2))))
                attn_rows = jnp.transpose(attn_heads, (1, 0, 2)).reshape(PATCH_ROWS, WIDTH)
                residual = hidden.astype(jnp.float32) + gate_attn * (jnp.dot(attn_rows, out_weight, preferred_element_type=jnp.float32) + bias_row[9 * WIDTH:10 * WIDTH])
                mlp_in = (layer_norm(residual) * (1.0 + scale_mlp) + shift_mlp).astype(jnp.bfloat16)
                mlp_mid = jax.nn.gelu(jnp.dot(mlp_in, up_weight, preferred_element_type=jnp.float32) + bias_row[10 * WIDTH:14 * WIDTH], approximate=True).astype(jnp.bfloat16)
                hidden = (residual + gate_mlp * (jnp.dot(mlp_mid, down_weight, preferred_element_type=jnp.float32) + bias_row[14 * WIDTH:])).astype(jnp.bfloat16)
                return hidden, (key_buf, value_buf)

            hidden = (jnp.dot(x_patch.astype(jnp.bfloat16), w_in, preferred_element_type=jnp.float32) + pos_embed[patch_idx].astype(jnp.float32)).astype(jnp.bfloat16)
            hidden, (key_all, value_all) = lax.scan(block, hidden, (mod_all, w_qkv, w_o, w_up, w_down, bias_f32, key_all, value_all))
            out_in = (layer_norm(hidden.astype(jnp.float32)) * (1.0 + scale_out) + shift_out).astype(jnp.bfloat16)
            velocity = jnp.dot(out_in, w_out, preferred_element_type=jnp.float32)
            return (key_all, value_all), x_patch + step_val * velocity

        (key_bufs, value_bufs), latent = lax.scan(patch_body, (key_bufs, value_bufs), jnp.arange(PATCHES))
    return latent
```

```python
import functools

import jax
import jax.numpy as jnp
from jax import lax
from jax.experimental import pallas as pl
from jax.experimental.pallas import tpu as pltpu
from jax.sharding import PartitionSpec as P

LN_EPS = 1e-6


def layer_norm(hidden):
    mean_val = jnp.mean(hidden, axis=-1, keepdims=True)
    centered = hidden - mean_val
    var_val = jnp.mean(centered * centered, axis=-1, keepdims=True)
    return centered * lax.rsqrt(var_val + LN_EPS)


def attend_kernel(head_dim, scale, q_ref, fresh_ref, kold_ref, vold_ref, out_ref):
    half = fresh_ref.shape[0] // 2
    first = pl.program_id(0) < pl.num_programs(0) // 2
    query = q_ref[:, :head_dim]
    key0 = fresh_ref[:half, head_dim:2 * head_dim]
    val0 = fresh_ref[:half, 2 * head_dim:]
    key1 = jnp.where(first, kold_ref[...], fresh_ref[half:, head_dim:2 * head_dim])
    val1 = jnp.where(first, vold_ref[...], fresh_ref[half:, 2 * head_dim:])
    dims = (((1,), (1,)), ((), ()))
    logit0 = lax.dot_general(query, key0, dims, preferred_element_type=jnp.float32) * scale
    logit1 = lax.dot_general(query, key1, dims, preferred_element_type=jnp.float32) * scale
    peak = jnp.maximum(jnp.max(logit0, axis=-1, keepdims=True), jnp.max(logit1, axis=-1, keepdims=True))
    exp0 = jnp.exp(logit0 - peak)
    exp1 = jnp.exp(logit1 - peak)
    total = jnp.sum(exp0, axis=-1, keepdims=True) + jnp.sum(exp1, axis=-1, keepdims=True)
    inv = 1.0 / total
    prob0 = (exp0 * inv).astype(jnp.bfloat16)
    prob1 = (exp1 * inv).astype(jnp.bfloat16)
    out = jnp.dot(prob0, val0, preferred_element_type=jnp.float32) + jnp.dot(prob1, val1, preferred_element_type=jnp.float32)
    out_ref[...] = out.astype(jnp.bfloat16)


def solution(mesh):
    stage_count = mesh.shape["pp"]
    split_count = mesh.shape["sp"]
    group = stage_count * split_count
    axes = ("pp", "sp")
    row_spec = P("dp", "sp", None)
    full_spec = P()
    buf_spec = P("dp", None, None, None)
    in_specs = (row_spec, P(None, "sp", None), P("dp", None), P("dp"), full_spec, full_spec, full_spec, full_spec, full_spec, full_spec, full_spec, full_spec, full_spec, full_spec, buf_spec, buf_spec)

    def device_fn(latent_in, pos_embed, condition, step_size, w_in, w_ada, w_qkv, w_o, w_up, w_down, b_layer, w_fa, b_fa, w_out, k_old, v_old):
        num_patches, sub_rows, _ = latent_in.shape
        width = w_in.shape[1]
        layers = w_qkv.shape[0]
        heads, head_dim = k_old.shape[2], k_old.shape[3]
        tokens = k_old.shape[1]
        patch_rows = tokens // num_patches
        per_patch = stage_count // num_patches
        rows = sub_rows // per_patch
        stage_idx = lax.axis_index("pp")
        me = stage_idx * split_count + lax.axis_index("sp")
        patch = stage_idx // per_patch
        start = (stage_idx % per_patch) * rows
        latent = lax.dynamic_slice(latent_in, (patch, start, 0), (1, rows, latent_in.shape[2]))[0]
        pos = lax.dynamic_slice(pos_embed, (patch, start, 0), (1, rows, width))[0].astype(jnp.float32)
        keys1 = lax.dynamic_slice(k_old, (0, patch_rows, me, 0), (layers, patch_rows, 1, head_dim))[:, :, 0]
        vals1 = lax.dynamic_slice(v_old, (0, patch_rows, me, 0), (layers, patch_rows, 1, head_dim))[:, :, 0]
        bias = b_layer.astype(jnp.float32)

        cond = jax.nn.silu(condition.astype(jnp.float32)).astype(jnp.bfloat16)
        pieces = group // layers
        piece = 6 * width // pieces
        w_mine = lax.dynamic_slice(w_ada, (me // pieces, 0, (me % pieces) * piece), (1, width, piece))[0]
        mod_mine = jnp.dot(cond, w_mine, preferred_element_type=jnp.float32)
        mod_all = lax.all_gather(mod_mine, axes, axis=0, tiled=False)
        mod_all = mod_all.reshape(layers, pieces, 2, piece).transpose(2, 0, 1, 3).reshape(2, layers, 6 * width) + bias[None, :, :6 * width]
        final_mod = jnp.dot(cond, w_fa, preferred_element_type=jnp.float32) + b_fa.astype(jnp.float32)

        blocks = 4
        attend = pl.pallas_call(
            functools.partial(attend_kernel, head_dim, head_dim ** -0.5),
            grid=(blocks,),
            out_shape=jax.ShapeDtypeStruct((tokens, head_dim), jnp.bfloat16),
            in_specs=[
                pl.BlockSpec((tokens // blocks, 3 * head_dim), lambda i: (i, 0)),
                pl.BlockSpec((tokens, 3 * head_dim), lambda i: (0, 0)),
                pl.BlockSpec((patch_rows, head_dim), lambda i: (0, 0)),
                pl.BlockSpec((patch_rows, head_dim), lambda i: (0, 0)),
            ],
            out_specs=pl.BlockSpec((tokens // blocks, head_dim), lambda i: (i, 0)),
            cost_estimate=pl.CostEstimate(flops=4 * tokens * tokens * head_dim, bytes_accessed=2 * tokens * 4 * head_dim, transcendentals=tokens * tokens),
        )

        keys1 = [keys1[layer] for layer in range(layers)]
        vals1 = [vals1[layer] for layer in range(layers)]
        for step in range(2):
            hidden = (jnp.dot(latent.astype(jnp.bfloat16), w_in, preferred_element_type=jnp.float32) + pos).astype(jnp.bfloat16)
            for layer in range(layers):
                row = bias[layer]
                s1, b1, g1, s2, b2, g2 = jnp.split(mod_all[step, layer], 6)
                normed = (layer_norm(hidden.astype(jnp.float32)) * (1.0 + s1) + b1).astype(jnp.bfloat16)
                qkv = (jnp.dot(normed, w_qkv[layer], preferred_element_type=jnp.float32) + row[6 * width:9 * width]).astype(jnp.bfloat16)
                send = qkv.reshape(rows, 3, heads, head_dim).transpose(2, 0, 1, 3).reshape(heads, rows, 3 * head_dim)
                fresh = lax.all_to_all(send, axes, split_axis=0, concat_axis=0, tiled=True).reshape(tokens, 3 * head_dim)
                out = attend(fresh, fresh, keys1[layer], vals1[layer])
                keys1[layer] = fresh[patch_rows:, head_dim:2 * head_dim]
                vals1[layer] = fresh[patch_rows:, 2 * head_dim:]
                back = lax.all_to_all(out.reshape(group, rows, head_dim), axes, split_axis=0, concat_axis=0, tiled=True)
                attn = back.transpose(1, 0, 2).reshape(rows, width)
                resid = hidden.astype(jnp.float32) + g1 * (jnp.dot(attn, w_o[layer], preferred_element_type=jnp.float32) + row[9 * width:10 * width])
                mlp_in = (layer_norm(resid) * (1.0 + s2) + b2).astype(jnp.bfloat16)
                mid = jax.nn.gelu(jnp.dot(mlp_in, w_up[layer], preferred_element_type=jnp.float32) + row[10 * width:14 * width], approximate=True).astype(jnp.bfloat16)
                hidden = (resid + g2 * (jnp.dot(mid, w_down[layer], preferred_element_type=jnp.float32) + row[14 * width:])).astype(jnp.bfloat16)
            s_out, b_out = jnp.split(final_mod[step], 2)
            normed = (layer_norm(hidden.astype(jnp.float32)) * (1.0 + s_out) + b_out).astype(jnp.bfloat16)
            latent = latent + step_size[step] * jnp.dot(normed, w_out, preferred_element_type=jnp.float32)
        return lax.all_gather(latent, "pp", axis=0, tiled=False).reshape(num_patches, sub_rows, latent.shape[-1])

    return jax.shard_map(device_fn, mesh=mesh, in_specs=in_specs, out_specs=row_spec, check_vma=False)
```

```python
import functools
import math

import jax
import jax.numpy as jnp
from jax import lax
from jax.experimental import pallas as pl
from jax.experimental.pallas import tpu as pltpu
from jax.sharding import PartitionSpec as P

LN_EPS = 1e-6
GROUP = 16
MESH = pl.DeviceIdType.MESH
ORDER = (15, 7, 14, 6, 13, 5, 12, 4, 11, 3, 10, 2, 9, 8, 1)


def layer_norm(hidden):
    mean_val = jnp.mean(hidden, axis=-1, keepdims=True)
    centered = hidden - mean_val
    var_val = jnp.mean(centered * centered, axis=-1, keepdims=True)
    return centered * lax.rsqrt(var_val + LN_EPS)


def step_kernel(dims, latent_ref, pos_ref, step_ref, w_in_ref, w_out_ref, mod_ref, fin_ref, bias_ref, kv_ref, w_qkv, w_o, w_up, w_down, out_ref,
                wq_v, wo_v, wu_v, wd_v, mods, cache, send, recv, obuf, back, qkv, attn, mid, hid, resid, xbuf, xall,
                w_sem, kv_sem, m_send, m_recv, q_send, q_recv, o_send, o_recv, x_send, x_recv):
    rows, width, layers, head_dim = dims
    bf16, f32 = jnp.bfloat16, jnp.float32
    dp, pp, sp = lax.axis_index("dp"), lax.axis_index("pp"), lax.axis_index("sp")
    zc, yc, cc = pp % 2, sp // 2, sp % 2
    image = pp // 2
    me = dp * 8 + zc * 4 + sp

    def peer_of(d):
        x, z, y, c = (dp + d // 8) % 2, (zc + (d // 4) % 2) % 2, (yc + (d // 2) % 2) % 2, (cc + d % 2) % 2
        s = y * 2 + c
        return x * 8 + z * 4 + s, (x, image * 2 + z, s)

    def place_of(g):
        return (g // 8, image * 2 + (g // 4) % 2, g % 4)

    barrier = pltpu.get_barrier_semaphore()
    for d in ORDER:
        pl.semaphore_signal(barrier, inc=1, device_id=peer_of(d)[1], device_id_type=MESH)
    for k in range(4):
        pl.semaphore_signal(barrier, inc=1, device_id=(k // 2, (1 - image) * 2 + k % 2, sp), device_id_type=MESH)

    def load(k, src, dst):
        return pltpu.make_async_copy(src, dst, w_sem.at[k])

    load(0, w_qkv.at[0], wq_v).start()
    kv_copy = pltpu.make_async_copy(kv_ref, cache, kv_sem)
    kv_copy.start()
    load(1, w_o.at[0], wo_v).start()
    load(2, w_up.at[0], wu_v).start()
    load(3, w_down.at[0], wd_v).start()
    pl.semaphore_wait(barrier, len(ORDER) + 4)

    def mod_copy(d):
        return pltpu.make_async_remote_copy(src_ref=mod_ref, dst_ref=mods.at[me], send_sem=m_send.at[d], recv_sem=m_recv.at[d], device_id=peer_of(d)[1], device_id_type=MESH)

    for d in ORDER:
        mod_copy(d).start()
    mods[me] = mod_ref[...]
    for d in ORDER:
        mod_copy(d).wait()

    lane = lax.broadcasted_iota(jnp.int32, (rows, 128), 1)
    low = lane < head_dim
    scale = head_dim ** -0.5 * math.log2(math.e)
    tdims = (((1,), (1,)), ((), ()))

    def qkv_copy(d, slot):
        peer, place = peer_of(d)
        return pltpu.make_async_remote_copy(src_ref=send.at[peer], dst_ref=recv.at[slot, me], send_sem=q_send.at[d], recv_sem=q_recv.at[slot, d], device_id=place, device_id_type=MESH)

    def own_copy(slot):
        return pltpu.make_async_copy(send.at[me], recv.at[slot, me], q_recv.at[slot, 0])

    def o_copy(g):
        return pltpu.make_async_remote_copy(src_ref=obuf.at[g], dst_ref=back.at[me], send_sem=o_send.at[g], recv_sem=o_recv.at[me], device_id=place_of(g), device_id_type=MESH)

    def own_back(g):
        return pltpu.make_async_copy(obuf.at[g], back.at[g], o_recv.at[g])

    def window(col):
        t, off = col // 128, col % 128
        if off == 0:
            return qkv[:, t * 128:t * 128 + 128]
        if off + head_dim <= 128:
            return pltpu.roll(qkv[:, t * 128:t * 128 + 128], 128 - off, 1)
        return pltpu.roll(qkv[:, t * 128:t * 128 + 256], 256 - off, 1)[:, :128]

    def layer_body(it, carry):
        layer = it % layers
        step = it // layers
        slot = it % 2
        nxt = (it + 1) % layers
        more = it + 1 < 2 * layers

        def mod(which, j):
            return mods[2 * layer + which, pl.ds(step * 3 + j, 1), :]

        @pl.when(layer == 0)
        def _():
            emb = jnp.dot(xbuf[...].astype(bf16), w_in_ref[...], preferred_element_type=f32) + pos_ref[...].astype(f32)
            hid[...] = emb.astype(bf16)

        normed = (layer_norm(hid[...].astype(f32)) * (1.0 + mod(0, 0)) + mod(0, 1)).astype(bf16)
        load(0, w_qkv.at[layer], wq_v).wait()

        def qkv_body(j, c):
            cols = pl.ds(pl.multiple_of(j * width, 128), width)
            qkv[:, cols] = jnp.dot(normed, wq_v[:, cols], preferred_element_type=f32) + bias_ref[layer, :, cols]
            return c
        lax.fori_loop(0, 3, qkv_body, 0)

        @pl.when(more)
        def _():
            load(0, w_qkv.at[nxt], wq_v).start()

        for g in range(GROUP):
            q, k, v = (window(part * width + g * head_dim) for part in range(3))
            send[g, :, :128] = jnp.where(low, q, pltpu.roll(v, head_dim, 1)).astype(bf16)
            send[g, :, 128:] = jnp.where(low, k, pltpu.roll(v, 2 * head_dim - 128, 1)).astype(bf16)
        for d in ORDER:
            qkv_copy(d, slot).start()
        own_copy(slot).start()

        @pl.when(it == 0)
        def _():
            kv_copy.wait()

        for d in ORDER:
            qkv_copy(d, slot).wait()
        own_copy(slot).wait()

        half = GROUP // 2
        for b in range(half):
            query = recv[slot, 2 * b:2 * b + 2, :, :128].reshape(2 * rows, 128)
            query = jnp.where(jnp.concatenate([low, low], axis=0), query.astype(f32), 0.0).astype(bf16)
            blk0 = recv[slot, :half].reshape(half * rows, 256)
            if b < half // 2:
                blk1 = cache[layer]
            else:
                blk1 = recv[slot, half:].reshape(half * rows, 256)
            log0 = lax.dot_general(query, blk0[:, 128:], tdims, preferred_element_type=f32)
            log1 = lax.dot_general(query, blk1[:, 128:], tdims, preferred_element_type=f32)
            peak = jnp.maximum(jnp.max(log0, axis=-1, keepdims=True), jnp.max(log1, axis=-1, keepdims=True))
            exp0 = jnp.exp2((log0 - peak) * scale)
            exp1 = jnp.exp2((log1 - peak) * scale)
            inv = 1.0 / (jnp.sum(exp0, axis=-1, keepdims=True) + jnp.sum(exp1, axis=-1, keepdims=True))
            out = jnp.dot((exp0 * inv).astype(bf16), blk0, preferred_element_type=f32) + jnp.dot((exp1 * inv).astype(bf16), blk1, preferred_element_type=f32)
            low2 = lax.broadcasted_iota(jnp.int32, (2 * rows, 128), 1) >= head_dim
            both = jnp.where(low2, out[:, :128], pltpu.roll(out[:, 128:], 128 - head_dim, 1))
            both = pltpu.roll(both, 128 - head_dim, 1).astype(bf16)
            obuf[2 * b:2 * b + 2] = both.reshape(2, rows, 128)
            for g in (2 * b, 2 * b + 1):
                @pl.when(me != g)
                def _():
                    o_copy(g).start()

                @pl.when(me == g)
                def _():
                    own_back(g).start()
        cache[layer] = recv[slot, half:].reshape(half * rows, 256)

        for g in range(GROUP):
            own_back(g).wait()
            attn[:, g * head_dim:(g + 1) * head_dim] = back[g, :, :head_dim]

        load(1, w_o.at[layer], wo_v).wait()
        proj = jnp.dot(attn[...], wo_v[...], preferred_element_type=f32) + bias_ref[layer, :, 3 * width:4 * width]
        res = hid[...].astype(f32) + mod(0, 2) * proj
        resid[...] = res

        @pl.when(more)
        def _():
            load(1, w_o.at[nxt], wo_v).start()

        mlp_in = (layer_norm(res) * (1.0 + mod(1, 0)) + mod(1, 1)).astype(bf16)
        load(2, w_up.at[layer], wu_v).wait()

        def up_body(j, c):
            cols = pl.ds(pl.multiple_of(j * width, 128), width)
            bcols = pl.ds(pl.multiple_of((j + 4) * width, 128), width)
            up = jnp.dot(mlp_in, wu_v[:, cols], preferred_element_type=f32) + bias_ref[layer, :, bcols]
            mid[j] = jax.nn.gelu(up, approximate=True).astype(bf16)
            return c
        lax.fori_loop(0, 4, up_body, 0)

        @pl.when(more)
        def _():
            load(2, w_up.at[nxt], wu_v).start()

        load(3, w_down.at[layer], wd_v).wait()

        def down_body(j, acc):
            return acc + jnp.dot(mid[j], wd_v[pl.ds(pl.multiple_of(j * width, 128), width), :], preferred_element_type=f32)
        down = lax.fori_loop(0, 4, down_body, jnp.zeros((rows, width), f32))
        hidden = (resid[...] + mod(1, 2) * (down + bias_ref[layer, :, 8 * width:9 * width])).astype(bf16)
        hid[...] = hidden

        @pl.when(more)
        def _():
            load(3, w_down.at[nxt], wd_v).start()

        for g in range(GROUP):
            @pl.when(me != g)
            def _():
                o_copy(g).wait_send()

        @pl.when(layer == layers - 1)
        def _():
            out_in = (layer_norm(hidden.astype(f32)) * (1.0 + fin_ref[step, 0:1, :]) + fin_ref[step, 1:2, :]).astype(bf16)
            vel = jnp.dot(out_in, w_out_ref[...], preferred_element_type=f32)
            xbuf[...] = xbuf[...] + step_ref[step] * vel
        return carry

    xbuf[...] = latent_ref[...]
    lax.fori_loop(0, 2 * layers, layer_body, 0)

    def x_copy(k):
        return pltpu.make_async_remote_copy(src_ref=xbuf, dst_ref=xall.at[dp * 2 + zc], send_sem=x_send.at[k], recv_sem=x_recv.at[dp * 2 + zc], device_id=(image, k, sp), device_id_type=MESH)

    own = pltpu.make_async_copy(xbuf, xall.at[dp * 2 + zc], x_recv.at[dp * 2 + zc])
    for k in range(4):
        mine = jnp.logical_and(image == dp, pp == k)

        @pl.when(jnp.logical_not(mine))
        def _():
            x_copy(k).start()

        @pl.when(mine)
        def _():
            own.start()
    for k in range(4):
        pltpu.make_async_copy(xbuf, xall.at[k], x_recv.at[k]).wait()
        mine = jnp.logical_and(image == dp, pp == k)

        @pl.when(jnp.logical_not(mine))
        def _():
            x_copy(k).wait_send()
    out_ref[...] = xall[...]


def solution(mesh):
    row_spec = P("dp", "sp", None)
    full_spec = P()
    buf_spec = P("dp", None, None, None)
    in_specs = (row_spec, P(None, "sp", None), P("dp", None), P("dp"), full_spec, full_spec, full_spec, full_spec, full_spec, full_spec, full_spec, full_spec, full_spec, full_spec, buf_spec, buf_spec)

    def device_fn(latent_in, pos_embed, condition, step_size, w_in, w_ada, w_qkv, w_o, w_up, w_down, b_layer, w_fa, b_fa, w_out, k_old, v_old):
        f32, bf16 = jnp.float32, jnp.bfloat16
        num_patches, sub_rows, patch_dim = latent_in.shape
        width = w_in.shape[1]
        layers = w_qkv.shape[0]
        head_dim = k_old.shape[3]
        patch_rows = k_old.shape[1] // num_patches
        rows = sub_rows // 2
        dp, pp, sp = lax.axis_index("dp"), lax.axis_index("pp"), lax.axis_index("sp")
        zc, image = pp % 2, pp // 2
        me = dp * 8 + zc * 4 + sp
        local = image == dp
        swap = [(0, 1), (1, 0)]

        def heads_of(buf, head):
            return lax.dynamic_slice(buf, (0, patch_rows, head, 0), (layers, patch_rows, 1, head_dim)).reshape(layers, patch_rows * head_dim // 128, 128)

        def rows_of(patch):
            return lax.dynamic_slice(latent_in, (patch, zc * rows, 0), (1, rows, patch_dim)).reshape(-1)

        other = (1 - dp) * 8 + zc * 4 + sp
        kv_send = jnp.concatenate([heads_of(k_old, other), heads_of(v_old, other)], axis=0)
        kv_got = lax.ppermute(kv_send, "dp", swap)
        kv_own = jnp.concatenate([heads_of(k_old, me), heads_of(v_old, me)], axis=0)
        small = jnp.concatenate([condition.astype(f32).reshape(-1), step_size])
        pack_got = lax.ppermute(jnp.concatenate([rows_of(1 - dp), small]), "dp", swap)
        pack = jnp.where(local, jnp.concatenate([rows_of(dp), small]), pack_got)
        latent = pack[:rows * patch_dim].reshape(rows, patch_dim)
        cond32 = pack[rows * patch_dim:rows * patch_dim + 2 * width].reshape(2, width)
        steps = jnp.broadcast_to(pack[-2:].reshape(2, 1, 1), (2, 1, patch_dim))
        pos = lax.dynamic_slice(pos_embed, (dp, zc * rows, 0), (1, rows, width))[0]

        cond = jax.nn.silu(cond32).astype(bf16)
        piece = 3 * width
        w_mine = lax.dynamic_slice(w_ada, (me // 2, 0, (me % 2) * piece), (1, width, piece))[0]
        b_mine = lax.dynamic_slice(b_layer, (me // 2, (me % 2) * piece), (1, piece)).astype(f32)
        mod_mine = (jnp.dot(cond, w_mine, preferred_element_type=f32) + b_mine).reshape(6, width)
        fin = (jnp.dot(cond, w_fa, preferred_element_type=f32) + b_fa.astype(f32)).reshape(2, 2, width)
        bias = b_layer[:, 6 * width:].astype(f32).reshape(layers, 1, 9 * width)

        kv = jnp.where(local, kv_own, kv_got).reshape(2, layers, patch_rows, head_dim)
        head_gap = 128 - head_dim
        kept = jnp.concatenate([jnp.zeros_like(kv[0]), kv[1, ..., :head_gap], kv[0], kv[1, ..., head_gap:], jnp.zeros((layers, patch_rows, 256 - 3 * head_dim), bf16)], axis=-1)

        vmem = pl.BlockSpec(memory_space=pltpu.VMEM)
        hbm = pl.BlockSpec(memory_space=pl.ANY)
        dma = pltpu.SemaphoreType.DMA
        out = pl.pallas_call(
            functools.partial(step_kernel, (rows, width, layers, head_dim)),
            out_shape=jax.ShapeDtypeStruct((4, rows, patch_dim), f32),
            in_specs=[vmem] * 8 + [hbm] * 5,
            out_specs=vmem,
            scratch_shapes=[
                pltpu.VMEM((width, 3 * width), bf16),
                pltpu.VMEM((width, width), bf16),
                pltpu.VMEM((width, 4 * width), bf16),
                pltpu.VMEM((4 * width, width), bf16),
                pltpu.VMEM((GROUP, 6, width), f32),
                pltpu.VMEM((layers, patch_rows, 256), bf16),
                pltpu.VMEM((GROUP, rows, 256), bf16),
                pltpu.VMEM((2, GROUP, rows, 256), bf16),
                pltpu.VMEM((GROUP, rows, 128), bf16),
                pltpu.VMEM((GROUP, rows, 128), bf16),
                pltpu.VMEM((rows, 3 * width), f32),
                pltpu.VMEM((rows, width), bf16),
                pltpu.VMEM((4, rows, width), bf16),
                pltpu.VMEM((rows, width), bf16),
                pltpu.VMEM((rows, width), f32),
                pltpu.VMEM((rows, patch_dim), f32),
                pltpu.VMEM((4, rows, patch_dim), f32),
                dma((4,)), dma, dma((GROUP,)), dma((GROUP,)), dma((GROUP,)), dma((2, GROUP)), dma((GROUP,)), dma((GROUP,)), dma((4,)), dma((4,)),
            ],
            compiler_params=pltpu.CompilerParams(collective_id=0, has_side_effects=True, vmem_limit_bytes=60 * 1024 * 1024),
        )(latent, pos, steps, w_in, w_out, mod_mine, fin, bias, kept, w_qkv, w_o, w_up, w_down)
        return out.reshape(num_patches, sub_rows, patch_dim)

    return jax.shard_map(device_fn, mesh=mesh, in_specs=in_specs, out_specs=row_spec, check_vma=False)
```

```python
import functools
import math

import jax
import jax.numpy as jnp
from jax import lax
from jax.experimental import pallas as pl
from jax.experimental.pallas import tpu as pltpu
from jax.sharding import PartitionSpec as P

LN_EPS = 1e-6
GROUP = 16
MESH = pl.DeviceIdType.MESH
ORDER = (15, 7, 14, 6, 13, 5, 12, 4, 11, 3, 10, 2, 9, 8, 1)


def layer_norm(hidden):
    mean_val = jnp.mean(hidden, axis=-1, keepdims=True)
    centered = hidden - mean_val
    var_val = jnp.mean(centered * centered, axis=-1, keepdims=True)
    return centered * lax.rsqrt(var_val + LN_EPS)


def step_kernel(dims, latent_ref, pos_ref, step_ref, w_in_ref, w_out_ref, mod_ref, fin_ref, bias_ref, k_pair, v_pair, w_qkv, w_o, w_up, w_down, out_ref,
                wq_v, wo_v, wu_v, wd_v, mods, cache, k_raw, v_raw, send, recv, obuf, back, qkv, attn, mid, hid, resid, xbuf, xall,
                w_sem, k_sem, v_sem, k_send, v_send, m_send, m_recv, q_send, q_recv, o_send, o_recv, x_send, x_recv):
    rows, width, layers, head_dim = dims
    bf16, f32 = jnp.bfloat16, jnp.float32
    dp, pp, sp = lax.axis_index("dp"), lax.axis_index("pp"), lax.axis_index("sp")
    zc, yc, cc = pp % 2, sp // 2, sp % 2
    image = pp // 2
    me = dp * 8 + zc * 4 + sp
    local = image == dp
    total = 2 * layers

    def peer_of(d):
        x, z, y, c = (dp + d // 8) % 2, (zc + (d // 4) % 2) % 2, (yc + (d // 2) % 2) % 2, (cc + d % 2) % 2
        s = y * 2 + c
        return x * 8 + z * 4 + s, (x, image * 2 + z, s)

    def place_of(g):
        return (g // 8, image * 2 + (g // 4) % 2, g % 4)

    barrier = pltpu.get_barrier_semaphore()
    for d in ORDER:
        pl.semaphore_signal(barrier, inc=1, device_id=peer_of(d)[1], device_id_type=MESH)
    for k in range(4):
        pl.semaphore_signal(barrier, inc=1, device_id=(k // 2, (1 - image) * 2 + k % 2, sp), device_id_type=MESH)

    def load(k, src, dst):
        return pltpu.make_async_copy(src, dst, w_sem.at[k])

    load(0, w_qkv.at[0], wq_v).start()
    load(1, w_o.at[0], wo_v).start()
    load(2, w_up.at[0], wu_v).start()
    load(3, w_down.at[0], wd_v).start()
    pl.semaphore_wait(barrier, len(ORDER) + 4)

    def mod_copy(d):
        return pltpu.make_async_remote_copy(src_ref=mod_ref, dst_ref=mods.at[me], send_sem=m_send.at[d], recv_sem=m_recv.at[d], device_id=peer_of(d)[1], device_id_type=MESH)

    for d in ORDER:
        mod_copy(d).start()
    mods[me] = mod_ref[...]

    def old_copies(layer):
        return (pltpu.make_async_copy(k_pair.at[dp, layer], k_raw.at[layer], k_sem.at[layer]),
                pltpu.make_async_copy(v_pair.at[dp, layer], v_raw.at[layer], v_sem.at[layer]))

    def old_sends(layer):
        there = (1 - dp, pp, sp)
        return (pltpu.make_async_remote_copy(src_ref=k_pair.at[1 - dp, layer], dst_ref=k_raw.at[layer], send_sem=k_send.at[layer], recv_sem=k_sem.at[layer], device_id=there, device_id_type=MESH),
                pltpu.make_async_remote_copy(src_ref=v_pair.at[1 - dp, layer], dst_ref=v_raw.at[layer], send_sem=v_send.at[layer], recv_sem=v_sem.at[layer], device_id=there, device_id_type=MESH))

    def old_start(layer):
        @pl.when(local)
        def _():
            for copy in old_sends(layer) + old_copies(layer):
                copy.start()

    old_start(0)
    for d in ORDER:
        mod_copy(d).wait()

    lane = lax.broadcasted_iota(jnp.int32, (rows, 128), 1)
    low = lane < head_dim
    scale = head_dim ** -0.5 * math.log2(math.e)
    tdims = (((1,), (1,)), ((), ()))

    def qkv_copy(p, d, slot):
        peer, place = peer_of(d)
        return pltpu.make_async_remote_copy(src_ref=send.at[p, peer], dst_ref=recv.at[p, slot, me], send_sem=q_send.at[p, d], recv_sem=q_recv.at[p, slot, d], device_id=place, device_id_type=MESH)

    def own_copy(p, slot):
        return pltpu.make_async_copy(send.at[p, me], recv.at[p, slot, me], q_recv.at[p, slot, 0])

    def o_copy(p, g):
        return pltpu.make_async_remote_copy(src_ref=obuf.at[p, g], dst_ref=back.at[p, me], send_sem=o_send.at[p, g], recv_sem=o_recv.at[p, me], device_id=place_of(g), device_id_type=MESH)

    def own_back(p, g):
        return pltpu.make_async_copy(obuf.at[p, g], back.at[p, g], o_recv.at[p, g])

    def window(col):
        t, off = col // 128, col % 128
        if off == 0:
            return qkv[:, t * 128:t * 128 + 128]
        if off + head_dim <= 128:
            return pltpu.roll(qkv[:, t * 128:t * 128 + 128], 128 - off, 1)
        return pltpu.roll(qkv[:, t * 128:t * 128 + 256], 256 - off, 1)[:, :128]

    def finish(p, it):
        layer = (it + layers - 1) % layers
        step = (it - 1) // layers
        nxt = it % layers
        refill = jnp.logical_and(p == 1, it < total)

        def mod(which, j):
            return mods[2 * layer + which, pl.ds(step * 3 + j, 1), :]

        for g in range(GROUP):
            own_back(p, g).wait()
            attn[:, g * head_dim:(g + 1) * head_dim] = back[p, g, :, :head_dim]
        if p == 0:
            load(1, w_o.at[layer], wo_v).wait()
        proj = jnp.dot(attn[...], wo_v[...], preferred_element_type=f32) + bias_ref[layer, :, 3 * width:4 * width]
        res = hid[p].astype(f32) + mod(0, 2) * proj
        resid[...] = res
        mlp_in = (layer_norm(res) * (1.0 + mod(1, 0)) + mod(1, 1)).astype(bf16)

        @pl.when(refill)
        def _():
            load(1, w_o.at[nxt], wo_v).start()

        if p == 0:
            load(2, w_up.at[layer], wu_v).wait()

        def up_body(j, c):
            cols = pl.ds(pl.multiple_of(j * width, 128), width)
            bcols = pl.ds(pl.multiple_of((j + 4) * width, 128), width)
            up = jnp.dot(mlp_in, wu_v[:, cols], preferred_element_type=f32) + bias_ref[layer, :, bcols]
            mid[j] = jax.nn.gelu(up, approximate=True).astype(bf16)
            return c
        lax.fori_loop(0, 4, up_body, 0)

        @pl.when(refill)
        def _():
            load(2, w_up.at[nxt], wu_v).start()

        if p == 0:
            load(3, w_down.at[layer], wd_v).wait()
        down = jnp.dot(jnp.concatenate([mid[j] for j in range(4)], axis=1), wd_v[...], preferred_element_type=f32)
        hidden = (resid[...] + mod(1, 2) * (down + bias_ref[layer, :, 8 * width:9 * width])).astype(bf16)
        hid[p] = hidden

        @pl.when(refill)
        def _():
            load(3, w_down.at[nxt], wd_v).start()

        for g in range(GROUP):
            @pl.when(me != g)
            def _():
                o_copy(p, g).wait_send()

        @pl.when(layer == layers - 1)
        def _():
            out_in = (layer_norm(hidden.astype(f32)) * (1.0 + fin_ref[step, 0:1, :]) + fin_ref[step, 1:2, :]).astype(bf16)
            vel = jnp.dot(out_in, w_out_ref[...], preferred_element_type=f32)
            xbuf[p] = xbuf[p] + step_ref[step] * vel

    def begin(p, it):
        layer = it % layers
        step = it // layers
        slot = it % 2

        def mod(which, j):
            return mods[2 * layer + which, pl.ds(step * 3 + j, 1), :]

        @pl.when(layer == 0)
        def _():
            emb = jnp.dot(xbuf[p].astype(bf16), w_in_ref[...], preferred_element_type=f32) + pos_ref[p].astype(f32)
            hid[p] = emb.astype(bf16)

        normed = (layer_norm(hid[p].astype(f32)) * (1.0 + mod(0, 0)) + mod(0, 1)).astype(bf16)
        if p == 0:
            load(0, w_qkv.at[layer], wq_v).wait()
        qkv[...] = jnp.dot(normed, wq_v[...], preferred_element_type=f32) + bias_ref[layer, :, :3 * width]

        if p == 1:
            @pl.when(it + 1 < total)
            def _():
                load(0, w_qkv.at[(it + 1) % layers], wq_v).start()

        for g in range(GROUP):
            q, k, v = (window(part * width + g * head_dim) for part in range(3))
            send[p, g, :, :128] = jnp.where(low, q, pltpu.roll(v, head_dim, 1)).astype(bf16)
            send[p, g, :, 128:] = jnp.where(low, k, pltpu.roll(v, 2 * head_dim - 128, 1)).astype(bf16)
        for d in ORDER:
            qkv_copy(p, d, slot).start()
        own_copy(p, slot).start()

    def attend(p, it):
        layer = it % layers
        slot = it % 2
        for d in ORDER:
            qkv_copy(p, d, slot).wait()
        own_copy(p, slot).wait()
        per = GROUP // 4
        wide = per * rows
        for fx, fz in ((1, 1), (1, 0), (0, 1), (0, 0)):
            block = (dp + fx) % 2 * 2 + (zc + fz) % 2
            query = recv[p, slot, pl.ds(block * per, per), :, :128].reshape(wide, 128)
            wide_lane = lax.broadcasted_iota(jnp.int32, (wide, 128), 1)
            query = jnp.where(wide_lane < head_dim, query.astype(f32), 0.0).astype(bf16)
            blk0 = recv[0, slot].reshape(GROUP * rows, 256)
            blk1 = cache[layer] if p == 0 else recv[1, slot].reshape(GROUP * rows, 256)
            log0 = lax.dot_general(query, blk0[:, 128:], tdims, preferred_element_type=f32)
            log1 = lax.dot_general(query, blk1[:, 128:], tdims, preferred_element_type=f32)
            peak = jnp.maximum(jnp.max(log0, axis=-1, keepdims=True), jnp.max(log1, axis=-1, keepdims=True))
            exp0 = jnp.exp2((log0 - peak) * scale)
            exp1 = jnp.exp2((log1 - peak) * scale)
            inv = 1.0 / (jnp.sum(exp0, axis=-1, keepdims=True) + jnp.sum(exp1, axis=-1, keepdims=True))
            out = jnp.dot((exp0 * inv).astype(bf16), blk0, preferred_element_type=f32) + jnp.dot((exp1 * inv).astype(bf16), blk1, preferred_element_type=f32)
            both = jnp.where(wide_lane >= head_dim, out[:, :128], pltpu.roll(out[:, 128:], 128 - head_dim, 1))
            both = pltpu.roll(both, 128 - head_dim, 1).astype(bf16)
            obuf[p, pl.ds(block * per, per)] = both.reshape(per, rows, 128)
            for i in range(per):
                g = block * per + i

                @pl.when(me != g)
                def _():
                    o_copy(p, g).start()

                @pl.when(me == g)
                def _():
                    own_back(p, g).start()

    def loop_body(it, carry):
        @pl.when(it < layers - 1)
        def _():
            old_start(it + 1)

        for p in range(2):
            @pl.when(it > 0)
            def _():
                finish(p, it)

            @pl.when(it < total)
            def _():
                begin(p, it)

        @pl.when(it < layers)
        def _():
            for copy in old_copies(it):
                copy.wait()
            for copy in old_sends(it):
                @pl.when(local)
                def _():
                    copy.wait_send()
            val = v_raw[it].astype(f32)
            old_lane = lax.broadcasted_iota(jnp.int32, val.shape, 1)
            cache[it, :, :128] = pltpu.roll(val, head_dim, 1).astype(bf16)
            cache[it, :, 128:] = jnp.where(old_lane < head_dim, k_raw[it].astype(f32), pltpu.roll(val, 2 * head_dim - 128, 1)).astype(bf16)

        @pl.when(it < total)
        def _():
            attend(0, it)
            attend(1, it)
            cache[it % layers] = recv[1, it % 2].reshape(GROUP * rows, 256)
        return carry

    xbuf[...] = latent_ref[...]
    lax.fori_loop(0, total + 1, loop_body, 0)

    def x_copy(k):
        return pltpu.make_async_remote_copy(src_ref=xbuf, dst_ref=xall.at[dp * 2 + zc], send_sem=x_send.at[k], recv_sem=x_recv.at[dp * 2 + zc], device_id=(image, k, sp), device_id_type=MESH)

    own = pltpu.make_async_copy(xbuf, xall.at[dp * 2 + zc], x_recv.at[dp * 2 + zc])
    for k in range(4):
        mine = jnp.logical_and(local, pp == k)

        @pl.when(jnp.logical_not(mine))
        def _():
            x_copy(k).start()

        @pl.when(mine)
        def _():
            own.start()
    for k in range(4):
        pltpu.make_async_copy(xbuf, xall.at[k], x_recv.at[k]).wait()
        mine = jnp.logical_and(local, pp == k)

        @pl.when(jnp.logical_not(mine))
        def _():
            x_copy(k).wait_send()
    for p in range(2):
        for k in range(4):
            out_ref[p, k * rows:(k + 1) * rows, :] = xall[k, p]


def solution(mesh):
    row_spec = P("dp", "sp", None)
    full_spec = P()
    buf_spec = P("dp", None, None, None)
    in_specs = (row_spec, P(None, "sp", None), P("dp", None), P("dp"), full_spec, full_spec, full_spec, full_spec, full_spec, full_spec, full_spec, full_spec, full_spec, full_spec, buf_spec, buf_spec)

    def device_fn(latent_in, pos_embed, condition, step_size, w_in, w_ada, w_qkv, w_o, w_up, w_down, b_layer, w_fa, b_fa, w_out, k_old, v_old):
        f32, bf16 = jnp.float32, jnp.bfloat16
        num_patches, sub_rows, patch_dim = latent_in.shape
        width = w_in.shape[1]
        layers = w_qkv.shape[0]
        head_dim = k_old.shape[3]
        patch_rows = k_old.shape[1] // num_patches
        rows = sub_rows // 4
        dp, pp, sp = lax.axis_index("dp"), lax.axis_index("pp"), lax.axis_index("sp")
        zc, image = pp % 2, pp // 2
        me = dp * 8 + zc * 4 + sp
        local = image == dp
        swap = [(0, 1), (1, 0)]

        def rows_of(quarter):
            return lax.dynamic_slice(latent_in, (0, quarter * rows, 0), (num_patches, rows, patch_dim)).reshape(-1)

        count = num_patches * rows * patch_dim
        small = jnp.concatenate([condition.astype(f32).reshape(-1), step_size])
        pack_got = lax.ppermute(jnp.concatenate([rows_of((1 - dp) * 2 + zc), small]), "dp", swap)
        pack = jnp.where(local, jnp.concatenate([rows_of(dp * 2 + zc), small]), pack_got)
        latent = pack[:count].reshape(num_patches, rows, patch_dim)
        cond32 = pack[count:count + 2 * width].reshape(2, width)
        steps = jnp.broadcast_to(pack[-2:].reshape(2, 1, 1), (2, 1, patch_dim))
        pos = lax.dynamic_slice(pos_embed, (0, (dp * 2 + zc) * rows, 0), (num_patches, rows, width))

        cond = jax.nn.silu(cond32).astype(bf16)
        piece = 3 * width
        w_mine = lax.dynamic_slice(w_ada, (me // 2, 0, (me % 2) * piece), (1, width, piece))[0]
        b_mine = lax.dynamic_slice(b_layer, (me // 2, (me % 2) * piece), (1, piece)).astype(f32)
        mod_mine = (jnp.dot(cond, w_mine, preferred_element_type=f32) + b_mine).reshape(6, width)
        fin = (jnp.dot(cond, w_fa, preferred_element_type=f32) + b_fa.astype(f32)).reshape(2, 2, width)
        bias = b_layer[:, 6 * width:].astype(f32).reshape(layers, 1, 9 * width)

        def heads_of(buf, head):
            part = lax.dynamic_slice(buf, (0, patch_rows, head, 0), (layers, patch_rows, 1, head_dim)).reshape(layers, patch_rows, head_dim)
            return jnp.pad(part, ((0, 0), (0, 0), (0, 128 - head_dim)))

        head = zc * 4 + sp
        k_pair = jnp.stack([heads_of(k_old, head), heads_of(k_old, head + 8)])
        v_pair = jnp.stack([heads_of(v_old, head), heads_of(v_old, head + 8)])

        vmem = pl.BlockSpec(memory_space=pltpu.VMEM)
        hbm = pl.BlockSpec(memory_space=pl.ANY)
        dma = pltpu.SemaphoreType.DMA
        return pl.pallas_call(
            functools.partial(step_kernel, (rows, width, layers, head_dim)),
            out_shape=jax.ShapeDtypeStruct((num_patches, sub_rows, patch_dim), f32),
            in_specs=[vmem] * 8 + [hbm] * 6,
            out_specs=vmem,
            scratch_shapes=[
                pltpu.VMEM((width, 3 * width), bf16),
                pltpu.VMEM((width, width), bf16),
                pltpu.VMEM((width, 4 * width), bf16),
                pltpu.VMEM((4 * width, width), bf16),
                pltpu.VMEM((GROUP, 6, width), f32),
                pltpu.VMEM((layers, patch_rows, 256), bf16),
                pltpu.VMEM((layers, patch_rows, 128), bf16),
                pltpu.VMEM((layers, patch_rows, 128), bf16),
                pltpu.VMEM((2, GROUP, rows, 256), bf16),
                pltpu.VMEM((2, 2, GROUP, rows, 256), bf16),
                pltpu.VMEM((2, GROUP, rows, 128), bf16),
                pltpu.VMEM((2, GROUP, rows, 128), bf16),
                pltpu.VMEM((rows, 3 * width), f32),
                pltpu.VMEM((rows, width), bf16),
                pltpu.VMEM((4, rows, width), bf16),
                pltpu.VMEM((2, rows, width), bf16),
                pltpu.VMEM((rows, width), f32),
                pltpu.VMEM((2, rows, patch_dim), f32),
                pltpu.VMEM((4, 2, rows, patch_dim), f32),
                dma((4,)), dma((layers,)), dma((layers,)), dma((layers,)), dma((layers,)), dma((GROUP,)), dma((GROUP,)), dma((2, GROUP)), dma((2, 2, GROUP)),
                dma((2, GROUP)), dma((2, GROUP)), dma((4,)), dma((4,)),
            ],
            compiler_params=pltpu.CompilerParams(collective_id=0, has_side_effects=True, vmem_limit_bytes=60 * 1024 * 1024),
        )(latent, pos, steps, w_in, w_out, mod_mine, fin, bias, k_pair, v_pair, w_qkv, w_o, w_up, w_down)

    return jax.shard_map(device_fn, mesh=mesh, in_specs=in_specs, out_specs=row_spec, check_vma=False)
```

```python
import functools
import math

import jax
import jax.numpy as jnp
from jax import lax
from jax.experimental import pallas as pl
from jax.experimental.pallas import tpu as pltpu
from jax.sharding import PartitionSpec as P

LN_EPS = 1e-6
GROUP = 16
MESH = pl.DeviceIdType.MESH
ORDER = (15, 7, 14, 6, 13, 5, 12, 4, 11, 3, 10, 2, 9, 8, 1)
CHIPS = (7, 3, 6, 2, 5, 1, 4)


def layer_norm(hidden):
    mean_val = jnp.mean(hidden, axis=-1, keepdims=True)
    centered = hidden - mean_val
    var_val = jnp.mean(centered * centered, axis=-1, keepdims=True)
    return centered * lax.rsqrt(var_val + LN_EPS)


def step_kernel(dims, latent_ref, pos_ref, step_ref, w_in_ref, w_out_ref, mod_ref, fin_ref, bias_ref, k_mine, v_mine, k_other, v_other, w_qkv, w_o, w_up, w_down, out_ref,
                wq_v, wo_v, wu_v, wd_v, mods, cache, k_raw, v_raw, pack, recv, obuf, back, qkv, attn, mid, hid, resid, xbuf, xall,
                w_sem, k_sem, v_sem, k_send, v_send, m_send, m_recv, q_send, q_recv, o_send, o_recv, d_send, d_recv, e_send, e_recv, x_send, x_recv):
    rows, width, layers, head_dim = dims
    bf16, f32 = jnp.bfloat16, jnp.float32
    dp, pp, sp = lax.axis_index("dp"), lax.axis_index("pp"), lax.axis_index("sp")
    zc, yc, cc = pp % 2, sp // 2, sp % 2
    image = pp // 2
    me = dp * 8 + zc * 4 + sp
    local = image == dp
    total = 2 * layers

    def peer_of(d):
        x, z, y, c = (dp + d // 8) % 2, (zc + (d // 4) % 2) % 2, (yc + (d // 2) % 2) % 2, (cc + d % 2) % 2
        s = y * 2 + c
        return x * 8 + z * 4 + s, (x, image * 2 + z, s)

    chip = dp * 4 + zc * 2 + yc
    partner = (dp, pp, yc * 2 + (1 - cc))

    def chip_of(d):
        x, z, y = (dp + d // 4) % 2, (zc + (d // 2) % 2) % 2, (yc + d % 2) % 2
        return x * 4 + z * 2 + y, (x, image * 2 + z, y * 2 + cc)

    barrier = pltpu.get_barrier_semaphore()
    for d in ORDER:
        pl.semaphore_signal(barrier, inc=1, device_id=peer_of(d)[1], device_id_type=MESH)
    for k in range(4):
        pl.semaphore_signal(barrier, inc=1, device_id=(k // 2, (1 - image) * 2 + k % 2, sp), device_id_type=MESH)

    def load(k, src, dst):
        return pltpu.make_async_copy(src, dst, w_sem.at[k])

    load(0, w_qkv.at[0], wq_v).start()
    load(1, w_o.at[0], wo_v).start()
    load(2, w_up.at[0], wu_v).start()
    load(3, w_down.at[0], wd_v).start()
    pl.semaphore_wait(barrier, len(ORDER) + 4)

    def mod_copy(d):
        return pltpu.make_async_remote_copy(src_ref=mod_ref, dst_ref=mods.at[me], send_sem=m_send.at[d], recv_sem=m_recv.at[d], device_id=peer_of(d)[1], device_id_type=MESH)

    for d in ORDER:
        mod_copy(d).start()
    mods[me] = mod_ref[...]

    def old_copies(layer):
        return (pltpu.make_async_copy(k_mine.at[layer], k_raw.at[layer], k_sem.at[layer]),
                pltpu.make_async_copy(v_mine.at[layer], v_raw.at[layer], v_sem.at[layer]))

    def old_sends(layer):
        there = (1 - dp, pp, sp)
        return (pltpu.make_async_remote_copy(src_ref=k_other.at[layer], dst_ref=k_raw.at[layer], send_sem=k_send.at[layer], recv_sem=k_sem.at[layer], device_id=there, device_id_type=MESH),
                pltpu.make_async_remote_copy(src_ref=v_other.at[layer], dst_ref=v_raw.at[layer], send_sem=v_send.at[layer], recv_sem=v_sem.at[layer], device_id=there, device_id_type=MESH))

    def old_start(layer):
        @pl.when(local)
        def _():
            for copy in old_sends(layer) + old_copies(layer):
                copy.start()

    old_start(0)
    for d in ORDER:
        mod_copy(d).wait()

    lane = lax.broadcasted_iota(jnp.int32, (rows, 128), 1)
    low = lane < head_dim
    scale = head_dim ** -0.5 * math.log2(math.e)
    tdims = (((1,), (1,)), ((), ()))

    both = pl.ds(0, 2)

    def qkv_swap(p):
        return pltpu.make_async_remote_copy(src_ref=pack.at[p, 2], dst_ref=pack.at[p, 1], send_sem=d_send.at[p], recv_sem=d_recv.at[p], device_id=partner, device_id_type=MESH)

    def qkv_copy(p, d, slot):
        there, place = chip_of(d)
        return pltpu.make_async_remote_copy(src_ref=pack.at[p, both, there], dst_ref=recv.at[p, slot, both, chip], send_sem=q_send.at[p, d], recv_sem=q_recv.at[p, slot, d], device_id=place, device_id_type=MESH)

    def o_copy(p, d):
        there, place = chip_of(d)
        return pltpu.make_async_remote_copy(src_ref=obuf.at[p, both, there], dst_ref=back.at[p, both, chip], send_sem=o_send.at[p, d], recv_sem=o_recv.at[p, d], device_id=place, device_id_type=MESH)

    def o_swap(p):
        return pltpu.make_async_remote_copy(src_ref=back.at[p, 1], dst_ref=back.at[p, 2], send_sem=e_send.at[p], recv_sem=e_recv.at[p], device_id=partner, device_id_type=MESH)

    def spread(p, it):
        slot = it % 2
        qkv_swap(p).wait()
        for d in CHIPS:
            qkv_copy(p, d, slot).start()
        recv[p, slot, :, chip] = pack[p, both, chip]

    def relay(p):
        for d in CHIPS:
            o_copy(p, d).wait()
        o_swap(p).start()

    def window(col):
        t, off = col // 128, col % 128
        if off == 0:
            return qkv[:, t * 128:t * 128 + 128]
        if off + head_dim <= 128:
            return pltpu.roll(qkv[:, t * 128:t * 128 + 128], 128 - off, 1)
        return pltpu.roll(qkv[:, t * 128:t * 128 + 256], 256 - off, 1)[:, :128]

    def finish(p, it):
        layer = (it + layers - 1) % layers
        step = (it - 1) // layers
        nxt = it % layers
        refill = jnp.logical_and(p == 1, it < total)

        def mod(which, j):
            return mods[2 * layer + which, pl.ds(step * 3 + j, 1), :]

        o_swap(p).wait()
        for g in range(GROUP):
            attn[:, g * head_dim:(g + 1) * head_dim] = back[p, (g + cc) % 2 * 2, g // 2, :, :head_dim]
        if p == 0:
            load(1, w_o.at[layer], wo_v).wait()
        proj = jnp.dot(attn[...], wo_v[...], preferred_element_type=f32) + bias_ref[layer, :, 3 * width:4 * width]
        res = hid[p].astype(f32) + mod(0, 2) * proj
        resid[...] = res
        if p == 1:
            @pl.when(it < total)
            def _():
                spread(0, it)
        mlp_in = (layer_norm(res) * (1.0 + mod(1, 0)) + mod(1, 1)).astype(bf16)

        @pl.when(refill)
        def _():
            load(1, w_o.at[nxt], wo_v).start()

        if p == 0:
            load(2, w_up.at[layer], wu_v).wait()

        def up_body(j, c):
            cols = pl.ds(pl.multiple_of(j * width, 128), width)
            bcols = pl.ds(pl.multiple_of((j + 4) * width, 128), width)
            up = jnp.dot(mlp_in, wu_v[:, cols], preferred_element_type=f32) + bias_ref[layer, :, bcols]
            mid[j] = jax.nn.gelu(up, approximate=True).astype(bf16)
            return c
        lax.fori_loop(0, 4, up_body, 0)

        @pl.when(refill)
        def _():
            load(2, w_up.at[nxt], wu_v).start()

        if p == 0:
            load(3, w_down.at[layer], wd_v).wait()
        down = jnp.dot(jnp.concatenate([mid[j] for j in range(4)], axis=1), wd_v[...], preferred_element_type=f32)
        hidden = (resid[...] + mod(1, 2) * (down + bias_ref[layer, :, 8 * width:9 * width])).astype(bf16)
        hid[p] = hidden

        @pl.when(refill)
        def _():
            load(3, w_down.at[nxt], wd_v).start()

        if p == 0:
            relay(1)

        @pl.when(layer == layers - 1)
        def _():
            out_in = (layer_norm(hidden.astype(f32)) * (1.0 + fin_ref[step, 0:1, :]) + fin_ref[step, 1:2, :]).astype(bf16)
            vel = jnp.dot(out_in, w_out_ref[...], preferred_element_type=f32)
            xbuf[p] = xbuf[p] + step_ref[step] * vel

    def begin(p, it):
        layer = it % layers
        step = it // layers
        slot = it % 2

        def mod(which, j):
            return mods[2 * layer + which, pl.ds(step * 3 + j, 1), :]

        @pl.when(layer == 0)
        def _():
            emb = jnp.dot(xbuf[p].astype(bf16), w_in_ref[...], preferred_element_type=f32) + pos_ref[p].astype(f32)
            hid[p] = emb.astype(bf16)

        normed = (layer_norm(hid[p].astype(f32)) * (1.0 + mod(0, 0)) + mod(0, 1)).astype(bf16)
        if p == 0:
            load(0, w_qkv.at[layer], wq_v).wait()
        qkv[...] = jnp.dot(normed, wq_v[...], preferred_element_type=f32) + bias_ref[layer, :, :3 * width]

        if p == 1:
            @pl.when(it + 1 < total)
            def _():
                load(0, w_qkv.at[(it + 1) % layers], wq_v).start()

        for g in range(GROUP):
            q, k, v = (window(part * width + g * head_dim) for part in range(3))
            place = (g + cc) % 2 * 2
            pack[p, place, g // 2, :, :128] = jnp.where(low, q, pltpu.roll(v, head_dim, 1)).astype(bf16)
            pack[p, place, g // 2, :, 128:] = jnp.where(low, k, pltpu.roll(v, 2 * head_dim - 128, 1)).astype(bf16)
        qkv_swap(p).start()

    def attend(p, it):
        layer = it % layers
        slot = it % 2
        for d in CHIPS:
            qkv_copy(p, d, slot).wait()
        wide = 4 * rows
        for fx, fz in ((1, 1), (1, 0), (0, 1), (0, 0)):
            block = (dp + fx) % 2 * 2 + (zc + fz) % 2
            query = recv[p, slot, :, pl.ds(block * 2, 2), :, :128].reshape(wide, 128)
            wide_lane = lax.broadcasted_iota(jnp.int32, (wide, 128), 1)
            query = jnp.where(wide_lane < head_dim, query.astype(f32), 0.0).astype(bf16)
            blk0 = recv[0, slot].reshape(GROUP * rows, 256)
            blk1 = cache[layer] if p == 0 else recv[1, slot].reshape(GROUP * rows, 256)
            log0 = lax.dot_general(query, blk0[:, 128:], tdims, preferred_element_type=f32)
            log1 = lax.dot_general(query, blk1[:, 128:], tdims, preferred_element_type=f32)
            peak = jnp.maximum(jnp.max(log0, axis=-1, keepdims=True), jnp.max(log1, axis=-1, keepdims=True))
            exp0 = jnp.exp2((log0 - peak) * scale)
            exp1 = jnp.exp2((log1 - peak) * scale)
            inv = 1.0 / (jnp.sum(exp0, axis=-1, keepdims=True) + jnp.sum(exp1, axis=-1, keepdims=True))
            out = jnp.dot((exp0 * inv).astype(bf16), blk0, preferred_element_type=f32) + jnp.dot((exp1 * inv).astype(bf16), blk1, preferred_element_type=f32)
            rolled = jnp.where(wide_lane >= head_dim, out[:, :128], pltpu.roll(out[:, 128:], 128 - head_dim, 1))
            obuf[p, :, pl.ds(block * 2, 2)] = pltpu.roll(rolled, 128 - head_dim, 1).astype(bf16).reshape(2, 2, rows, 128)
            for fy in (1, 0):
                d = fx * 4 + fz * 2 + fy
                if d:
                    o_copy(p, d).start()
                else:
                    back[p, both, chip] = obuf[p, :, chip]

    def loop_body(it, carry):
        @pl.when(it < layers - 1)
        def _():
            old_start(it + 1)

        @pl.when(it > 0)
        def _():
            relay(0)

        for p in range(2):
            @pl.when(it > 0)
            def _():
                finish(p, it)

            if p == 1:
                @pl.when(it == 0)
                def _():
                    spread(0, it)

            @pl.when(it < total)
            def _():
                begin(p, it)

        @pl.when(it < layers)
        def _():
            for copy in old_copies(it):
                copy.wait()
            for copy in old_sends(it):
                @pl.when(local)
                def _():
                    copy.wait_send()
            gap = 128 - head_dim
            val = v_raw[it]
            cache[it, :, :128] = jnp.concatenate([jnp.zeros_like(val), val[:, :gap]], axis=1)
            cache[it, :, 128:] = jnp.concatenate([k_raw[it], val[:, gap:], jnp.zeros((val.shape[0], 256 - 3 * head_dim), bf16)], axis=1)

        @pl.when(it < total)
        def _():
            spread(1, it)
            attend(0, it)
            attend(1, it)
            cache[it % layers] = recv[1, it % 2].reshape(GROUP * rows, 256)
        return carry

    xbuf[...] = latent_ref[...]
    lax.fori_loop(0, total + 1, loop_body, 0)

    def x_copy(k):
        return pltpu.make_async_remote_copy(src_ref=xbuf, dst_ref=xall.at[dp * 2 + zc], send_sem=x_send.at[k], recv_sem=x_recv.at[dp * 2 + zc], device_id=(image, k, sp), device_id_type=MESH)

    own = pltpu.make_async_copy(xbuf, xall.at[dp * 2 + zc], x_recv.at[dp * 2 + zc])
    for k in range(4):
        mine = jnp.logical_and(local, pp == k)

        @pl.when(jnp.logical_not(mine))
        def _():
            x_copy(k).start()

        @pl.when(mine)
        def _():
            own.start()
    for k in range(4):
        pltpu.make_async_copy(xbuf, xall.at[k], x_recv.at[k]).wait()
        mine = jnp.logical_and(local, pp == k)

        @pl.when(jnp.logical_not(mine))
        def _():
            x_copy(k).wait_send()
    for p in range(2):
        for k in range(4):
            out_ref[p, k * rows:(k + 1) * rows, :] = xall[k, p]


def solution(mesh):
    row_spec = P("dp", "sp", None)
    full_spec = P()
    buf_spec = P("dp", None, None, None)
    in_specs = (row_spec, P(None, "sp", None), P("dp", None), P("dp"), full_spec, full_spec, full_spec, full_spec, full_spec, full_spec, full_spec, full_spec, full_spec, full_spec, buf_spec, buf_spec)

    def device_fn(latent_in, pos_embed, condition, step_size, w_in, w_ada, w_qkv, w_o, w_up, w_down, b_layer, w_fa, b_fa, w_out, k_old, v_old):
        f32, bf16 = jnp.float32, jnp.bfloat16
        num_patches, sub_rows, patch_dim = latent_in.shape
        width = w_in.shape[1]
        layers = w_qkv.shape[0]
        head_dim = k_old.shape[3]
        patch_rows = k_old.shape[1] // num_patches
        rows = sub_rows // 4
        dp, pp, sp = lax.axis_index("dp"), lax.axis_index("pp"), lax.axis_index("sp")
        zc, image = pp % 2, pp // 2
        me = dp * 8 + zc * 4 + sp
        local = image == dp
        swap = [(0, 1), (1, 0)]

        def rows_of(quarter):
            return lax.dynamic_slice(latent_in, (0, quarter * rows, 0), (num_patches, rows, patch_dim)).reshape(-1)

        count = num_patches * rows * patch_dim
        small = jnp.concatenate([condition.astype(f32).reshape(-1), step_size])
        pack_got = lax.ppermute(jnp.concatenate([rows_of((1 - dp) * 2 + zc), small]), "dp", swap)
        pack = jnp.where(local, jnp.concatenate([rows_of(dp * 2 + zc), small]), pack_got)
        latent = pack[:count].reshape(num_patches, rows, patch_dim)
        cond32 = pack[count:count + 2 * width].reshape(2, width)
        steps = jnp.broadcast_to(pack[-2:].reshape(2, 1, 1), (2, 1, patch_dim))
        pos = lax.dynamic_slice(pos_embed, (0, (dp * 2 + zc) * rows, 0), (num_patches, rows, width))

        cond = jax.nn.silu(cond32).astype(bf16)
        piece = 3 * width
        w_mine = lax.dynamic_slice(w_ada, (me // 2, 0, (me % 2) * piece), (1, width, piece))[0]
        b_mine = lax.dynamic_slice(b_layer, (me // 2, (me % 2) * piece), (1, piece)).astype(f32)
        mod_mine = (jnp.dot(cond, w_mine, preferred_element_type=f32) + b_mine).reshape(6, width)
        fin = (jnp.dot(cond, w_fa, preferred_element_type=f32) + b_fa.astype(f32)).reshape(2, 2, width)
        bias = b_layer[:, 6 * width:].astype(f32).reshape(layers, 1, 9 * width)

        def heads_of(buf, head):
            return lax.dynamic_slice(buf, (0, patch_rows, head, 0), (layers, patch_rows, 1, head_dim)).reshape(layers, patch_rows, head_dim)

        other = (1 - dp) * 8 + zc * 4 + sp
        olds = [heads_of(k_old, me), heads_of(v_old, me), heads_of(k_old, other), heads_of(v_old, other)]

        vmem = pl.BlockSpec(memory_space=pltpu.VMEM)
        hbm = pl.BlockSpec(memory_space=pl.ANY)
        dma = pltpu.SemaphoreType.DMA
        return pl.pallas_call(
            functools.partial(step_kernel, (rows, width, layers, head_dim)),
            out_shape=jax.ShapeDtypeStruct((num_patches, sub_rows, patch_dim), f32),
            in_specs=[vmem] * 8 + [hbm] * 8,
            out_specs=vmem,
            scratch_shapes=[
                pltpu.VMEM((width, 3 * width), bf16),
                pltpu.VMEM((width, width), bf16),
                pltpu.VMEM((width, 4 * width), bf16),
                pltpu.VMEM((4 * width, width), bf16),
                pltpu.VMEM((GROUP, 6, width), f32),
                pltpu.VMEM((layers, patch_rows, 256), bf16),
                pltpu.VMEM((layers, patch_rows, head_dim), bf16),
                pltpu.VMEM((layers, patch_rows, head_dim), bf16),
                pltpu.VMEM((2, 3, 8, rows, 256), bf16),
                pltpu.VMEM((2, 2, 2, 8, rows, 256), bf16),
                pltpu.VMEM((2, 2, 8, rows, 128), bf16),
                pltpu.VMEM((2, 3, 8, rows, 128), bf16),
                pltpu.VMEM((rows, 3 * width), f32),
                pltpu.VMEM((rows, width), bf16),
                pltpu.VMEM((4, rows, width), bf16),
                pltpu.VMEM((2, rows, width), bf16),
                pltpu.VMEM((rows, width), f32),
                pltpu.VMEM((2, rows, patch_dim), f32),
                pltpu.VMEM((4, 2, rows, patch_dim), f32),
                dma((4,)), dma((layers,)), dma((layers,)), dma((layers,)), dma((layers,)), dma((GROUP,)), dma((GROUP,)), dma((2, 8)), dma((2, 2, 8)),
                dma((2, 8)), dma((2, 8)), dma((2,)), dma((2,)), dma((2,)), dma((2,)), dma((4,)), dma((4,)),
            ],
            compiler_params=pltpu.CompilerParams(collective_id=0, has_side_effects=True, vmem_limit_bytes=60 * 1024 * 1024),
        )(latent, pos, steps, w_in, w_out, mod_mine, fin, bias, *olds, w_qkv, w_o, w_up, w_down)

    return jax.shard_map(device_fn, mesh=mesh, in_specs=in_specs, out_specs=row_spec, check_vma=False)
```

```python
import functools
import math

import jax
import jax.numpy as jnp
from jax import lax
from jax.experimental import pallas as pl
from jax.experimental.pallas import tpu as pltpu
from jax.sharding import PartitionSpec as P

LN_EPS = 1e-6
GROUP = 16
MESH = pl.DeviceIdType.MESH
ORDER = (15, 7, 14, 6, 13, 5, 12, 4, 11, 3, 10, 2, 9, 8, 1)
CHIPS = (7, 3, 6, 2, 5, 1, 4)


def layer_norm(hidden):
    mean_val = jnp.mean(hidden, axis=-1, keepdims=True)
    centered = hidden - mean_val
    var_val = jnp.mean(centered * centered, axis=-1, keepdims=True)
    return centered * lax.rsqrt(var_val + LN_EPS)


def step_kernel(dims, latent_ref, pos_ref, step_ref, w_in_ref, w_out_ref, mod_ref, fin_ref, bias_ref, k_mine, v_mine, k_other, v_other, w_qkv, w_o, w_up, w_down, out_ref,
                wq_v, wo_v, wu_v, wd_v, mods, cache, k_raw, v_raw, pack, recv, obuf, back, qkv, attn, mid, hid, resid, xbuf, xall,
                w_sem, k_sem, v_sem, k_send, v_send, m_send, m_recv, q_send, q_recv, o_send, o_recv, d_send, d_recv, e_send, e_recv, x_send, x_recv):
    rows, width, layers, head_dim = dims
    bf16, f32 = jnp.bfloat16, jnp.float32
    dp, pp, sp = lax.axis_index("dp"), lax.axis_index("pp"), lax.axis_index("sp")
    zc, yc, cc = pp % 2, sp // 2, sp % 2
    image = pp // 2
    me = dp * 8 + zc * 4 + sp
    local = image == dp
    total = 2 * layers

    def peer_of(d):
        x, z, y, c = (dp + d // 8) % 2, (zc + (d // 4) % 2) % 2, (yc + (d // 2) % 2) % 2, (cc + d % 2) % 2
        s = y * 2 + c
        return x * 8 + z * 4 + s, (x, image * 2 + z, s)

    chip = dp * 4 + zc * 2 + yc
    partner = (dp, pp, yc * 2 + (1 - cc))

    def chip_of(d):
        x, z, y = (dp + d // 4) % 2, (zc + (d // 2) % 2) % 2, (yc + d % 2) % 2
        return x * 4 + z * 2 + y, (x, image * 2 + z, y * 2 + cc)

    barrier = pltpu.get_barrier_semaphore()
    for d in ORDER:
        pl.semaphore_signal(barrier, inc=1, device_id=peer_of(d)[1], device_id_type=MESH)
    for k in range(4):
        pl.semaphore_signal(barrier, inc=1, device_id=(k // 2, (1 - image) * 2 + k % 2, sp), device_id_type=MESH)

    def load(k, src, dst):
        return pltpu.make_async_copy(src, dst, w_sem.at[k])

    load(0, w_qkv.at[0], wq_v).start()
    load(1, w_o.at[0], wo_v).start()
    load(2, w_up.at[0], wu_v).start()
    load(3, w_down.at[0], wd_v).start()
    pl.semaphore_wait(barrier, len(ORDER) + 4)

    def mod_copy(d):
        return pltpu.make_async_remote_copy(src_ref=mod_ref, dst_ref=mods.at[me], send_sem=m_send.at[d], recv_sem=m_recv.at[d], device_id=peer_of(d)[1], device_id_type=MESH)

    for d in ORDER:
        mod_copy(d).start()
    mods[me] = mod_ref[...]

    def old_copies(layer):
        return (pltpu.make_async_copy(k_mine.at[layer], k_raw.at[layer], k_sem.at[layer]),
                pltpu.make_async_copy(v_mine.at[layer], v_raw.at[layer], v_sem.at[layer]))

    def old_sends(layer):
        there = (1 - dp, pp, sp)
        return (pltpu.make_async_remote_copy(src_ref=k_other.at[layer], dst_ref=k_raw.at[layer], send_sem=k_send.at[layer], recv_sem=k_sem.at[layer], device_id=there, device_id_type=MESH),
                pltpu.make_async_remote_copy(src_ref=v_other.at[layer], dst_ref=v_raw.at[layer], send_sem=v_send.at[layer], recv_sem=v_sem.at[layer], device_id=there, device_id_type=MESH))

    def old_start(layer):
        @pl.when(local)
        def _():
            for copy in old_sends(layer) + old_copies(layer):
                copy.start()

    old_start(0)
    for d in ORDER:
        mod_copy(d).wait()

    lane = lax.broadcasted_iota(jnp.int32, (rows, 128), 1)
    low = lane < head_dim
    scale = head_dim ** -0.5 * math.log2(math.e)
    tdims = (((1,), (1,)), ((), ()))

    both = pl.ds(0, 2)

    def qkv_swap(p):
        return pltpu.make_async_remote_copy(src_ref=pack.at[p, 2], dst_ref=pack.at[p, 1], send_sem=d_send.at[p], recv_sem=d_recv.at[p], device_id=partner, device_id_type=MESH)

    def qkv_copy(p, d, slot):
        there, place = chip_of(d)
        return pltpu.make_async_remote_copy(src_ref=pack.at[p, both, there], dst_ref=recv.at[p, slot, both, chip], send_sem=q_send.at[p, d], recv_sem=q_recv.at[p, slot, d], device_id=place, device_id_type=MESH)

    def o_copy(p, d):
        there, place = chip_of(d)
        return pltpu.make_async_remote_copy(src_ref=obuf.at[p, both, there], dst_ref=back.at[p, both, chip], send_sem=o_send.at[p, d], recv_sem=o_recv.at[p, d], device_id=place, device_id_type=MESH)

    def o_swap(p):
        return pltpu.make_async_remote_copy(src_ref=back.at[p, 1], dst_ref=back.at[p, 2], send_sem=e_send.at[p], recv_sem=e_recv.at[p], device_id=partner, device_id_type=MESH)

    def spread(p, it):
        slot = it % 2
        qkv_swap(p).wait()
        for d in CHIPS:
            qkv_copy(p, d, slot).start()
        recv[p, slot, :, chip] = pack[p, both, chip]

    def relay(p):
        for d in CHIPS:
            o_copy(p, d).wait()
        o_swap(p).start()

    def window(col):
        t, off = col // 128, col % 128
        if off == 0:
            return qkv[:, t * 128:t * 128 + 128]
        if off + head_dim <= 128:
            return pltpu.roll(qkv[:, t * 128:t * 128 + 128], 128 - off, 1)
        return pltpu.roll(qkv[:, t * 128:t * 128 + 256], 256 - off, 1)[:, :128]

    def finish(p, it):
        layer = (it + layers - 1) % layers
        step = (it - 1) // layers
        nxt = it % layers
        refill = jnp.logical_and(p == 1, it < total)

        def mod(which, j):
            return mods[2 * layer + which, pl.ds(step * 3 + j, 1), :]

        o_swap(p).wait()
        for g in range(GROUP):
            attn[:, g * head_dim:(g + 1) * head_dim] = back[p, (g + cc) % 2 * 2, g // 2, :, :head_dim]
        if p == 0:
            load(1, w_o.at[layer], wo_v).wait()
        proj = jnp.dot(attn[...], wo_v[...], preferred_element_type=f32) + bias_ref[layer, :, 3 * width:4 * width]
        res = hid[p].astype(f32) + mod(0, 2) * proj
        resid[...] = res
        if p == 1:
            @pl.when(it < total)
            def _():
                spread(0, it)
        mlp_in = (layer_norm(res) * (1.0 + mod(1, 0)) + mod(1, 1)).astype(bf16)

        @pl.when(refill)
        def _():
            load(1, w_o.at[nxt], wo_v).start()

        if p == 0:
            load(2, w_up.at[layer], wu_v).wait()

        def up_body(j, c):
            cols = pl.ds(pl.multiple_of(j * width, 128), width)
            bcols = pl.ds(pl.multiple_of((j + 4) * width, 128), width)
            up = jnp.dot(mlp_in, wu_v[:, cols], preferred_element_type=f32) + bias_ref[layer, :, bcols]
            mid[j] = jax.nn.gelu(up, approximate=True).astype(bf16)

            @pl.when(refill)
            def _():
                load(2, w_up.at[nxt, :, cols], wu_v.at[:, cols]).start()
            return c
        lax.fori_loop(0, 4, up_body, 0)

        if p == 0:
            load(3, w_down.at[layer], wd_v).wait()
        down = jnp.dot(jnp.concatenate([mid[j] for j in range(4)], axis=1), wd_v[...], preferred_element_type=f32)
        hidden = (resid[...] + mod(1, 2) * (down + bias_ref[layer, :, 8 * width:9 * width])).astype(bf16)
        hid[p] = hidden

        if p == 0:
            relay(1)

        @pl.when(layer == layers - 1)
        def _():
            out_in = (layer_norm(hidden.astype(f32)) * (1.0 + fin_ref[step, 0:1, :]) + fin_ref[step, 1:2, :]).astype(bf16)
            vel = jnp.dot(out_in, w_out_ref[...], preferred_element_type=f32)
            xbuf[p] = xbuf[p] + step_ref[step] * vel

    def begin(p, it):
        layer = it % layers
        step = it // layers
        slot = it % 2

        def mod(which, j):
            return mods[2 * layer + which, pl.ds(step * 3 + j, 1), :]

        @pl.when(layer == 0)
        def _():
            emb = jnp.dot(xbuf[p].astype(bf16), w_in_ref[...], preferred_element_type=f32) + pos_ref[p].astype(f32)
            hid[p] = emb.astype(bf16)

        normed = (layer_norm(hid[p].astype(f32)) * (1.0 + mod(0, 0)) + mod(0, 1)).astype(bf16)
        if p == 0:
            load(0, w_qkv.at[layer], wq_v).wait()
        qkv[...] = jnp.dot(normed, wq_v[...], preferred_element_type=f32) + bias_ref[layer, :, :3 * width]

        for g in range(GROUP):
            q, k, v = (window(part * width + g * head_dim) for part in range(3))
            place = (g + cc) % 2 * 2
            pack[p, place, g // 2, :, :128] = jnp.where(low, q, pltpu.roll(v, head_dim, 1)).astype(bf16)
            pack[p, place, g // 2, :, 128:] = jnp.where(low, k, pltpu.roll(v, 2 * head_dim - 128, 1)).astype(bf16)
        qkv_swap(p).start()

    def attend(p, it):
        layer = it % layers
        slot = it % 2
        for d in CHIPS:
            qkv_copy(p, d, slot).wait()
        wide = 8 * rows
        for fx in (1, 0):
            first = (dp + fx) % 2 * 4
            part = pl.ds((2 * p + 1 - fx) * width, width)

            @pl.when(it > 0)
            def _():
                load(3, w_down.at[layer, part], wd_v.at[part]).start()

            query = recv[p, slot, :, pl.ds(first, 4), :, :128].reshape(wide, 128)
            wide_lane = lax.broadcasted_iota(jnp.int32, (wide, 128), 1)
            query = jnp.where(wide_lane < head_dim, query.astype(f32), 0.0).astype(bf16)
            blk0 = recv[0, slot].reshape(GROUP * rows, 256)
            blk1 = cache[layer] if p == 0 else recv[1, slot].reshape(GROUP * rows, 256)
            log0 = lax.dot_general(query, blk0[:, 128:], tdims, preferred_element_type=f32)
            log1 = lax.dot_general(query, blk1[:, 128:], tdims, preferred_element_type=f32)
            peak = jnp.maximum(jnp.max(log0, axis=-1, keepdims=True), jnp.max(log1, axis=-1, keepdims=True))
            exp0 = jnp.exp2((log0 - peak) * scale)
            exp1 = jnp.exp2((log1 - peak) * scale)
            inv = 1.0 / (jnp.sum(exp0, axis=-1, keepdims=True) + jnp.sum(exp1, axis=-1, keepdims=True))
            out = jnp.dot((exp0 * inv).astype(bf16), blk0, preferred_element_type=f32) + jnp.dot((exp1 * inv).astype(bf16), blk1, preferred_element_type=f32)
            rolled = jnp.where(wide_lane >= head_dim, out[:, :128], pltpu.roll(out[:, 128:], 128 - head_dim, 1))
            obuf[p, :, pl.ds(first, 4)] = pltpu.roll(rolled, 128 - head_dim, 1).astype(bf16).reshape(2, 4, rows, 128)
            for near in (3, 2, 1, 0):
                d = fx * 4 + near
                if d:
                    o_copy(p, d).start()
                else:
                    back[p, both, chip] = obuf[p, :, chip]

    def loop_body(it, carry):
        @pl.when(it < layers - 1)
        def _():
            old_start(it + 1)

        @pl.when(it > 0)
        def _():
            relay(0)

        for p in range(2):
            @pl.when(it > 0)
            def _():
                finish(p, it)

            if p == 1:
                @pl.when(it == 0)
                def _():
                    spread(0, it)

            @pl.when(it < total)
            def _():
                begin(p, it)

        @pl.when(it < layers)
        def _():
            for copy in old_copies(it):
                copy.wait()
            for copy in old_sends(it):
                @pl.when(local)
                def _():
                    copy.wait_send()
            gap = 128 - head_dim
            val = v_raw[it]
            cache[it, :, :128] = jnp.concatenate([jnp.zeros_like(val), val[:, :gap]], axis=1)
            cache[it, :, 128:] = jnp.concatenate([k_raw[it], val[:, gap:], jnp.zeros((val.shape[0], 256 - 3 * head_dim), bf16)], axis=1)

        @pl.when(it < total)
        def _():
            spread(1, it)
            attend(0, it)
            attend(1, it)

            @pl.when(it + 1 < total)
            def _():
                load(0, w_qkv.at[(it + 1) % layers], wq_v).start()

            cache[it % layers] = recv[1, it % 2].reshape(GROUP * rows, 256)
        return carry

    xbuf[...] = latent_ref[...]
    lax.fori_loop(0, total + 1, loop_body, 0)

    def x_copy(k):
        return pltpu.make_async_remote_copy(src_ref=xbuf, dst_ref=xall.at[dp * 2 + zc], send_sem=x_send.at[k], recv_sem=x_recv.at[dp * 2 + zc], device_id=(image, k, sp), device_id_type=MESH)

    own = pltpu.make_async_copy(xbuf, xall.at[dp * 2 + zc], x_recv.at[dp * 2 + zc])
    for k in range(4):
        mine = jnp.logical_and(local, pp == k)

        @pl.when(jnp.logical_not(mine))
        def _():
            x_copy(k).start()

        @pl.when(mine)
        def _():
            own.start()
    for k in range(4):
        pltpu.make_async_copy(xbuf, xall.at[k], x_recv.at[k]).wait()
        mine = jnp.logical_and(local, pp == k)

        @pl.when(jnp.logical_not(mine))
        def _():
            x_copy(k).wait_send()
    for p in range(2):
        for k in range(4):
            out_ref[p, k * rows:(k + 1) * rows, :] = xall[k, p]


def solution(mesh):
    row_spec = P("dp", "sp", None)
    full_spec = P()
    buf_spec = P("dp", None, None, None)
    in_specs = (row_spec, P(None, "sp", None), P("dp", None), P("dp"), full_spec, full_spec, full_spec, full_spec, full_spec, full_spec, full_spec, full_spec, full_spec, full_spec, buf_spec, buf_spec)

    def device_fn(latent_in, pos_embed, condition, step_size, w_in, w_ada, w_qkv, w_o, w_up, w_down, b_layer, w_fa, b_fa, w_out, k_old, v_old):
        f32, bf16 = jnp.float32, jnp.bfloat16
        num_patches, sub_rows, patch_dim = latent_in.shape
        width = w_in.shape[1]
        layers = w_qkv.shape[0]
        head_dim = k_old.shape[3]
        patch_rows = k_old.shape[1] // num_patches
        rows = sub_rows // 4
        dp, pp, sp = lax.axis_index("dp"), lax.axis_index("pp"), lax.axis_index("sp")
        zc, image = pp % 2, pp // 2
        me = dp * 8 + zc * 4 + sp
        local = image == dp
        swap = [(0, 1), (1, 0)]

        def rows_of(quarter):
            return lax.dynamic_slice(latent_in, (0, quarter * rows, 0), (num_patches, rows, patch_dim)).reshape(-1)

        count = num_patches * rows * patch_dim
        small = jnp.concatenate([condition.astype(f32).reshape(-1), step_size])
        pack_got = lax.ppermute(jnp.concatenate([rows_of((1 - dp) * 2 + zc), small]), "dp", swap)
        pack = jnp.where(local, jnp.concatenate([rows_of(dp * 2 + zc), small]), pack_got)
        latent = pack[:count].reshape(num_patches, rows, patch_dim)
        cond32 = pack[count:count + 2 * width].reshape(2, width)
        steps = jnp.broadcast_to(pack[-2:].reshape(2, 1, 1), (2, 1, patch_dim))
        pos = lax.dynamic_slice(pos_embed, (0, (dp * 2 + zc) * rows, 0), (num_patches, rows, width))

        cond = jax.nn.silu(cond32).astype(bf16)
        piece = 3 * width
        w_mine = lax.dynamic_slice(w_ada, (me // 2, 0, (me % 2) * piece), (1, width, piece))[0]
        b_mine = lax.dynamic_slice(b_layer, (me // 2, (me % 2) * piece), (1, piece)).astype(f32)
        mod_mine = (jnp.dot(cond, w_mine, preferred_element_type=f32) + b_mine).reshape(6, width)
        fin = (jnp.dot(cond, w_fa, preferred_element_type=f32) + b_fa.astype(f32)).reshape(2, 2, width)
        bias = b_layer[:, 6 * width:].astype(f32).reshape(layers, 1, 9 * width)

        def heads_of(buf, head):
            return lax.dynamic_slice(buf, (0, patch_rows, head, 0), (layers, patch_rows, 1, head_dim)).reshape(layers, patch_rows, head_dim)

        other = (1 - dp) * 8 + zc * 4 + sp
        olds = [heads_of(k_old, me), heads_of(v_old, me), heads_of(k_old, other), heads_of(v_old, other)]

        vmem = pl.BlockSpec(memory_space=pltpu.VMEM)
        hbm = pl.BlockSpec(memory_space=pl.ANY)
        dma = pltpu.SemaphoreType.DMA
        return pl.pallas_call(
            functools.partial(step_kernel, (rows, width, layers, head_dim)),
            out_shape=jax.ShapeDtypeStruct((num_patches, sub_rows, patch_dim), f32),
            in_specs=[vmem] * 8 + [hbm] * 8,
            out_specs=vmem,
            scratch_shapes=[
                pltpu.VMEM((width, 3 * width), bf16),
                pltpu.VMEM((width, width), bf16),
                pltpu.VMEM((width, 4 * width), bf16),
                pltpu.VMEM((4 * width, width), bf16),
                pltpu.VMEM((GROUP, 6, width), f32),
                pltpu.VMEM((layers, patch_rows, 256), bf16),
                pltpu.VMEM((layers, patch_rows, head_dim), bf16),
                pltpu.VMEM((layers, patch_rows, head_dim), bf16),
                pltpu.VMEM((2, 3, 8, rows, 256), bf16),
                pltpu.VMEM((2, 2, 2, 8, rows, 256), bf16),
                pltpu.VMEM((2, 2, 8, rows, 128), bf16),
                pltpu.VMEM((2, 3, 8, rows, 128), bf16),
                pltpu.VMEM((rows, 3 * width), f32),
                pltpu.VMEM((rows, width), bf16),
                pltpu.VMEM((4, rows, width), bf16),
                pltpu.VMEM((2, rows, width), bf16),
                pltpu.VMEM((rows, width), f32),
                pltpu.VMEM((2, rows, patch_dim), f32),
                pltpu.VMEM((4, 2, rows, patch_dim), f32),
                dma((4,)), dma((layers,)), dma((layers,)), dma((layers,)), dma((layers,)), dma((GROUP,)), dma((GROUP,)), dma((2, 8)), dma((2, 2, 8)),
                dma((2, 8)), dma((2, 8)), dma((2,)), dma((2,)), dma((2,)), dma((2,)), dma((4,)), dma((4,)),
            ],
            compiler_params=pltpu.CompilerParams(collective_id=0, has_side_effects=True, vmem_limit_bytes=60 * 1024 * 1024),
        )(latent, pos, steps, w_in, w_out, mod_mine, fin, bias, *olds, w_qkv, w_o, w_up, w_down)

    return jax.shard_map(device_fn, mesh=mesh, in_specs=in_specs, out_specs=row_spec, check_vma=False)
```
